256 devices in a mesh: rows: 32 (over z, y_lo, core), cols: 8 (over x, y_hi).
Axes of the slice: x: 4, y: 4 (y_hi: 2, y_lo: 2; y = y_hi * 2 + y_lo), z: 8, core: 2. Of those that a mesh axis runs over, the one named last changes fastest.
Arguments:
- matrix: float32 [8192, 8192], P('rows', 'cols'), may hold values from -6 to 6
- starts: int32 [4, 4], replicated, may hold values from 0 to 7936, as said below
- factors: float32 [4, 4, 256, 256], P(None, None, 'rows', 'cols'), as said below
Outputs:
- updated: float32 [8192, 8192], P('rows', 'cols')
The draws below stay inside these ranges and needn't reach their ends.
Inputs may be any that keep to these rules, and one draw needn't show every extreme that they name: `starts`: every start is a multiple of 128; chain c's start lies in the c-th of 4 equal ranges of blocks and never decreases from advance to advance; a window may end on the first block of the next range; the windows of one advance are disjoint. `factors`: every factor is orthogonal.
All inputs are finite; a program needn't handle non-finite values.
Results may differ from the reference program's by a relative error of at most 0.0001.
Values sent between devices are 32-bit elements; how exact they have to be, the bound alone decides.
No kernel may reach another device: no remote copies, remote signals or barrier semaphores. Data moves between devices by JAX's collectives and lax.ppermute only.
A program may use at most 64 MiB of HBM per device.

```python
import jax
import jax.numpy as jnp
from jax import lax

N = 8192
NB = 128
CHAINS = 4
ADV = 4
W = 256
N_ROWS = 32
N_COLS = 8


def draw_starts(key, part):
    region = N // NB // CHAINS
    first_row = jnp.zeros((1, CHAINS), jnp.int32)
    middle_rows = jax.random.randint(jax.random.fold_in(key, 11), (ADV - 2, CHAINS), 1, region - 1)
    middle_rows = jnp.sort(middle_rows, axis=0).astype(jnp.int32)
    chain_ids = jnp.arange(CHAINS, dtype=jnp.int32)
    last_row = jnp.where(chain_ids == CHAINS - 1, region - 2, region - 1).astype(jnp.int32)[None, :]
    offsets = jnp.concatenate([first_row, middle_rows, last_row], axis=0)
    bases = chain_ids * region
    return ((bases[None, :] + offsets) * NB).astype(jnp.int32)


def draw_factors(key, part):
    gauss_draw = jax.random.normal(jax.random.fold_in(key, 23), (ADV, CHAINS, W, W), jnp.float32)
    orthog, upper = jnp.linalg.qr(gauss_draw)
    signs = jnp.where(jnp.diagonal(upper, axis1=-2, axis2=-1) >= 0.0, 1.0, -1.0)
    return (orthog * signs[..., None, :]).astype(jnp.float32)


def levels(own_key, dims, cuts, least, largest):
    level = 1.0
    for position, shards_of in cuts:
        steps = jax.random.uniform(jax.random.fold_in(jax.random.fold_in(own_key, 6), position), (shards_of,), jnp.float32, least / len(cuts), largest / len(cuts))
        level = level * jnp.repeat(jnp.exp(steps), dims[position] // shards_of).reshape((-1,) + (1,) * (len(dims) - 1 - position))
    return level


def gaussian(rng, shape, spread, limit, cuts=(), held_as=jnp.bfloat16):
    drawn = jax.random.normal(rng, shape, jnp.float32) * spread
    if len(cuts) > 0:
        drawn = levels(rng, shape, cuts, -0.22, 0.18) * drawn
    return jnp.clip(drawn, min=-limit, max=limit).astype(held_as)


def setup_inputs(seed: int = 0) -> dict:
    streams_of = jax.random.split(jax.random.key(seed), 4)
    matrix = gaussian(streams_of[0], (N, N), 1.0, 6.0, ((0, 32), (1, 8)), jnp.float32)
    starts = draw_starts(jax.random.fold_in(streams_of[3], 71), 0)
    factors = draw_factors(jax.random.fold_in(streams_of[3], 71), 0)
    return {"matrix": matrix, "starts": starts, "factors": factors}


def to_natural(source):
    rows_per = N // (N_ROWS * NB)
    cols_per = N // (N_COLS * NB)
    source = source.reshape(N_ROWS, rows_per, NB, N).transpose(1, 0, 2, 3).reshape(N, N)
    return source.reshape(N, N_COLS, cols_per, NB).transpose(0, 2, 1, 3).reshape(N, N)

def to_stored(source):
    rows_per = N // (N_ROWS * NB)
    cols_per = N // (N_COLS * NB)
    source = source.reshape(rows_per, N_ROWS, NB, N).transpose(1, 0, 2, 3).reshape(N, N)
    return source.reshape(N, cols_per, N_COLS, NB).transpose(0, 2, 1, 3).reshape(N, N)

def reference(matrix, starts, factors):
    active = to_natural(matrix)
    for advance in range(ADV):
        for chain_id in range(CHAINS):
            offset = starts[advance, chain_id].astype(jnp.int32)
            factor = factors[advance, chain_id]
            window_rows = lax.dynamic_slice_in_dim(active, offset, W, 0)
            changed = jnp.dot(factor.T.astype(jnp.float32), window_rows.astype(jnp.float32), precision=lax.Precision.HIGHEST, preferred_element_type=jnp.float32)
            active = lax.dynamic_update_slice_in_dim(active, changed, offset, 0)
        for chain_id in range(CHAINS):
            offset = starts[advance, chain_id].astype(jnp.int32)
            factor = factors[advance, chain_id]
            window_cols = lax.dynamic_slice_in_dim(active, offset, W, 1)
            changed = jnp.dot(window_cols.astype(jnp.float32), factor.astype(jnp.float32), precision=lax.Precision.HIGHEST, preferred_element_type=jnp.float32)
            active = lax.dynamic_update_slice_in_dim(active, changed, offset, 1)
    return to_stored(active)
```

```python
import jax
import jax.numpy as jnp
from jax import lax
from jax.experimental import pallas as pl
from jax.experimental.pallas import tpu as pltpu
from jax.sharding import PartitionSpec as P

NB = 128
CHAINS = 4
ADV = 4
ROWS = 32
COLS = 8
EACH = 32


def pack_kernel(tile, factors, out):
    lane_tiles = tile.shape[1] // NB
    for s in range(lane_tiles):
        for t in range(tile.shape[0] // NB):
            block = tile[t * NB : (t + 1) * NB, s * NB : (s + 1) * NB].T
            out[4 * s : 4 * s + 4, :EACH, t * NB : (t + 1) * NB] = block.reshape(4, EACH, NB)
    for half in range(2):
        pieces = [factors[2 * half + a, c] for a in range(2) for c in range(CHAINS)]
        piece = jnp.concatenate(pieces, axis=1)
        for d in range(half, 4 * lane_tiles, 2):
            out[d, EACH:, :] = piece


def pack(tile, factors):
    step = 256
    return pl.pallas_call(
        pack_kernel,
        grid=(tile.shape[1] // step,),
        in_specs=[
            pl.BlockSpec((256, step), lambda i: (0, i)),
            pl.BlockSpec((ADV, CHAINS, 8, 32), lambda i: (0, 0, 0, 0)),
        ],
        out_specs=pl.BlockSpec((step // EACH, EACH + 8, 256), lambda i: (i, 0, 0)),
        out_shape=jax.ShapeDtypeStruct((ROWS, EACH + 8, 256), jnp.float32),
        name="pack",
    )(tile, factors)


def spread_kernel(pieces, out):
    turned = pieces[...].reshape(256, 256).T
    for e in range(COLS):
        out[e] = turned


def spread(got):
    return pl.pallas_call(
        spread_kernel,
        grid=(1,),
        in_specs=[pl.BlockSpec((ROWS, 8, 256), lambda i: (0, EACH // 8, 0))],
        out_specs=pl.BlockSpec((COLS, 256, 256), lambda i: (0, 0, 0)),
        out_shape=jax.ShapeDtypeStruct((COLS, 256, 256), jnp.float32),
        name="spread",
    )(got)


def split(x):
    high = x.astype(jnp.bfloat16)
    return high, (x - high.astype(jnp.float32)).astype(jnp.bfloat16)


def times_factor(panel, turned_factor):
    dims = (((1,), (1,)), ((), ()))
    p_high, p_low = split(panel)
    u_high, u_low = split(turned_factor)
    both = jnp.concatenate([p_high, p_low], axis=0)
    first = lax.dot_general(both, u_high, dims, preferred_element_type=jnp.float32)
    second = lax.dot_general(p_high, u_low, dims, preferred_element_type=jnp.float32)
    return first[:EACH] + (first[EACH:] + second)


def apply_windows(panel, count, starts, core, own, other):
    def place(block):
        return lax.rem(block, count), pl.multiple_of(lax.div(block, count) * NB, NB)

    for k in range(ADV):
        is_own = core[0] == k // 2
        results = []
        for c in range(CHAINS):
            head = lax.div(starts[k, c], NB)
            p0, o0 = place(head)
            p1, o1 = place(head + 1)
            window = jnp.concatenate(
                [panel[p0, :, pl.ds(o0, NB)], panel[p1, :, pl.ds(o1, NB)]], axis=1
            )
            at = ((k % 2) * CHAINS + c) * 32
            factor = jnp.where(is_own, own[:, at : at + 32, :], other[:, at : at + 32, :])
            results.append((p0, o0, p1, o1, times_factor(window, factor.reshape(256, 256))))
        for p0, o0, p1, o1, new in results:
            panel[p0, :, pl.ds(o0, NB)] = new[:, :NB]
            panel[p1, :, pl.ds(o1, NB)] = new[:, NB:]


def swap_groups(parts):
    a0, a1, a2, a3 = parts
    axis = a0.ndim - 1
    lane = lax.broadcasted_iota(jnp.int32, a0.shape, axis)
    low = lane < 64
    even = lax.rem(lane, 64) < 32

    def roll(x, by):
        return pltpu.roll(x, by, axis)

    b0 = jnp.where(low, a0, roll(a2, 64))
    b2 = jnp.where(low, roll(a0, 64), a2)
    b1 = jnp.where(low, a1, roll(a3, 64))
    b3 = jnp.where(low, roll(a1, 64), a3)
    return (
        jnp.where(even, b0, roll(b1, 32)),
        jnp.where(even, roll(b0, 96), b1),
        jnp.where(even, b2, roll(b3, 32)),
        jnp.where(even, roll(b2, 96), b3),
    )


def row_kernel(starts, core, data, own, other, out, panel):
    panel[...] = data[...]
    apply_windows(panel, ROWS, starts, core, own, other)
    for t in range(ROWS // 4):
        for slot in range(2):
            block = panel[4 * t : 4 * t + 4, :, slot * NB : (slot + 1) * NB]
            turned = block.reshape(NB, NB).T.reshape(4, 4, 8, NB)
            parts = swap_groups([turned[:, g] for g in range(4)])
            for j in range(4):
                out[4 * t + j, 4 * slot : 4 * slot + 4] = parts[j]


def col_kernel(starts, core, data, own, other, out):
    for s in range(ROWS // 4):
        parts = swap_groups([data[4 * s + j] for j in range(4)])
        for g in range(4):
            out[:, 8 * g : 8 * g + 8, s * NB : (s + 1) * NB] = parts[g]
    apply_windows(out, COLS, starts, core, own, other)


SCALAR = pl.BlockSpec(memory_space=pltpu.SMEM)


def whole(*shape):
    return pl.BlockSpec(shape, lambda i: (0,) * len(shape))


def local(matrix, starts, factors):
    core = lax.rem(lax.axis_index("rows"), 2).reshape(1)
    packed = pack(matrix, factors)
    got = lax.all_to_all(packed, "rows", 0, 0, tiled=True)
    own = lax.all_to_all(spread(got), "cols", 0, 0, tiled=True)
    other = lax.ppermute(own, "rows", [(d, d ^ 1) for d in range(ROWS)])
    sent = pl.pallas_call(
        row_kernel,
        grid=(1,),
        in_specs=[SCALAR, SCALAR, whole(ROWS, EACH, 256)] + [whole(COLS, 256, 256)] * 2,
        out_specs=whole(ROWS, COLS, 8, NB),
        out_shape=jax.ShapeDtypeStruct((ROWS, COLS, 8, NB), jnp.float32),
        scratch_shapes=[pltpu.VMEM((ROWS, EACH, 256), jnp.float32)],
        name="row_windows",
    )(starts, core, got, own, other)
    sent = sent.reshape(ROWS * COLS, 8, NB)
    came = lax.all_to_all(sent, ("rows", "cols"), 0, 0, tiled=True)
    done = pl.pallas_call(
        col_kernel,
        grid=(1,),
        in_specs=[SCALAR, SCALAR, whole(ROWS, COLS, 8, NB)] + [whole(COLS, 256, 256)] * 2,
        out_specs=whole(COLS, EACH, 1024),
        out_shape=jax.ShapeDtypeStruct((COLS, EACH, 1024), jnp.float32),
        name="col_windows",
    )(starts, core, came.reshape(ROWS, COLS, 8, NB), own, other)
    home = lax.all_to_all(done, "cols", 0, 0, tiled=True)
    return home.reshape(256, 1024)


def solution(mesh):
    in_specs = (P("rows", "cols"), P(), P(None, None, "rows", "cols"))
    return jax.shard_map(
        local, mesh=mesh, in_specs=in_specs, out_specs=P("rows", "cols"), check_vma=False
    )
```

```python
import jax
import jax.numpy as jnp
from jax import lax
from jax.experimental import pallas as pl
from jax.experimental.pallas import tpu as pltpu
from jax.sharding import Mesh
from jax.sharding import PartitionSpec as P


NB = 128
CHAINS = 4
ADV = 4
PLANES = 8
QUADS = 4
COLS = 8
EACH = 32
WIDE = 256


def pieces_kernel(factors, out):
    for half in range(2):
        pieces = [factors[2 * half + a, c] for a in range(2) for c in range(CHAINS)]
        piece = jnp.concatenate(pieces, axis=1)
        for d in range(half, PLANES * QUADS, 2):
            out[d] = piece


def spread_kernel(pieces, out):
    turned = pieces[...].reshape(WIDE, WIDE).T
    for e in range(COLS):
        out[e] = turned


def split(x):
    high = x.astype(jnp.bfloat16)
    return high, (x - high.astype(jnp.float32)).astype(jnp.bfloat16)


def turned_factor(k, c, core, own, other):
    at = ((k % 2) * CHAINS + c) * 32
    picked = jnp.where(core == k // 2, own[:, at : at + 32, :], other[:, at : at + 32, :])
    return split(picked.reshape(WIDE, WIDE))


def dot(a, b, b_dim):
    return lax.dot_general(a, b, (((1,), (b_dim,)), ((), ())), preferred_element_type=jnp.float32)


def row_pass(panel, first, last, starts, place, own, other):
    for k in range(ADV):
        for c in range(CHAINS):
            offset = lax.div(starts[k, c], NB) + 1 - QUADS * place[2]
            slot = (offset >= PLANES * QUADS).astype(jnp.int32)
            head = offset - PLANES * QUADS * slot

            @pl.when((head >= first) & (head <= last))
            def _():
                f_high, f_low = turned_factor(k, c, place[0], own, other)
                window = jnp.concatenate([panel[head, slot], panel[head + 1, slot]], axis=0)
                w_high, w_low = split(window)
                new = dot(f_high, w_high, 0) + (dot(f_low, w_high, 0) + dot(f_high, w_low, 0))
                panel[head, slot] = new[:NB]
                panel[head + 1, slot] = new[NB:]


def load_plane(panel, blocks, place):
    for m, block in enumerate(blocks):
        panel[(place[1] ^ m) + 1] = block[...]


def edge_kernel(starts, place, b0, b1, b2, b3, own, other, up, down, panel):
    load_plane(panel, (b0, b1, b2, b3), place)
    down[...] = panel[1]
    row_pass(panel, 1, 3, starts, place, own, other)
    up[...] = panel[4]

    @pl.when(lax.rem(place[2], PLANES // 2) == 0)
    def _():
        down[...] = panel[1]


def row_kernel(starts, place, b0, b1, b2, b3, below, above, own, other, out, panel):
    load_plane(panel, (b0, b1, b2, b3), place)
    panel[0] = below[...]
    panel[5] = above[...]

    @pl.when(place[2] == 0)
    def _():
        panel[0, 1] = below[0]

    @pl.when(place[2] == PLANES - 1)
    def _():
        panel[5, 0] = above[1]

    row_pass(panel, 0, 4, starts, place, own, other)
    out[...] = panel[1:5]


def col_kernel(starts, place, data, own, other, out):
    for q in range(QUADS):
        out[:, :, q * WIDE : (q + 1) * WIDE] = data[q]

    def spot(block):
        return lax.rem(block, COLS), pl.multiple_of(lax.div(block, COLS) * NB, NB)

    for k in range(ADV):
        results = []
        for c in range(CHAINS):
            head = lax.div(starts[k, c], NB)
            e0, o0 = spot(head)
            e1, o1 = spot(head + 1)
            window = jnp.concatenate([out[e0, :, pl.ds(o0, NB)], out[e1, :, pl.ds(o1, NB)]], axis=1)
            w_high, w_low = split(window)
            f_high, f_low = turned_factor(k, c, place[0], own, other)
            both = dot(jnp.concatenate([w_high, w_low], axis=0), f_high, 1)
            new = both[:EACH] + (both[EACH:] + dot(w_high, f_low, 1))
            results.append((e0, o0, e1, o1, new))
        for e0, o0, e1, o1, new in results:
            out[e0, :, pl.ds(o0, NB)] = new[:, :NB]
            out[e1, :, pl.ds(o1, NB)] = new[:, NB:]


SCALARS = pl.BlockSpec(memory_space=pltpu.SMEM)
VALUES = pl.BlockSpec(memory_space=pltpu.VMEM)


def kernel(body, scalars, inputs, out_shapes, scratch=()):
    outs = [jax.ShapeDtypeStruct(shape, jnp.float32) for shape in out_shapes]
    return pl.pallas_call(
        body,
        in_specs=[SCALARS] * scalars + [VALUES] * inputs,
        out_specs=[VALUES] * len(outs),
        out_shape=outs,
        scratch_shapes=[pltpu.VMEM(shape, jnp.float32) for shape in scratch],
    )


def local(matrix, starts, factors):
    z = lax.axis_index("planes")
    q = lax.axis_index("quads")
    place = jnp.stack([lax.rem(q, 2), q, z])
    tile = matrix.reshape(2, NB, QUADS * WIDE)
    quarters = [lax.dynamic_slice_in_dim(tile, (q ^ m) * WIDE, WIDE, 2) for m in range(QUADS)]
    blocks = [quarters[0]]
    for m in range(1, QUADS):
        blocks.append(lax.ppermute(quarters[m], "quads", [(i, i ^ m) for i in range(QUADS)]))
    (sent,) = kernel(pieces_kernel, 0, 1, [(PLANES * QUADS, 8, WIDE)])(factors)
    got = lax.all_to_all(sent, ("planes", "quads"), 0, 0, tiled=True)
    (sent,) = kernel(spread_kernel, 0, 1, [(COLS, WIDE, WIDE)])(got)
    own = lax.all_to_all(sent, "cols", 0, 0, tiled=True)
    other = lax.ppermute(own, "quads", [(i, i ^ 1) for i in range(QUADS)])
    panel = (QUADS + 2, 2, NB, WIDE)
    up, down = kernel(edge_kernel, 2, 6, [(2, NB, WIDE)] * 2, [panel])(
        starts, place, *blocks, own, other
    )
    below = lax.ppermute(up, "planes", [(i, (i + 1) % PLANES) for i in range(PLANES)])
    above = lax.ppermute(down, "planes", [(i, (i - 1) % PLANES) for i in range(PLANES)])
    (rows,) = kernel(row_kernel, 2, 8, [(QUADS, 2, NB, WIDE)], [panel])(
        starts, place, *blocks, below, above, own, other
    )
    rows = rows.reshape(QUADS * COLS, EACH, WIDE)
    came = lax.all_to_all(rows, ("quads", "cols"), 0, 0, tiled=True)
    came = came.reshape(QUADS, COLS, EACH, WIDE)
    (done,) = kernel(col_kernel, 2, 3, [(COLS, EACH, QUADS * WIDE)])(
        starts, place, came, own, other
    )
    home = lax.all_to_all(done, "cols", 0, 0, tiled=True)
    return home.reshape(2 * NB, QUADS * WIDE)


def solution(mesh):
    finer = Mesh(mesh.devices.reshape(PLANES, QUADS, COLS), ("planes", "quads", "cols"))
    rows = ("planes", "quads")
    in_specs = (P(rows, "cols"), P(), P(None, None, rows, "cols"))
    return jax.shard_map(
        local, mesh=finer, in_specs=in_specs, out_specs=P(rows, "cols"), check_vma=False
    )
```

```python
import jax
import jax.numpy as jnp
from jax import lax
from jax.experimental import pallas as pl
from jax.experimental.pallas import tpu as pltpu
from jax.sharding import Mesh
from jax.sharding import PartitionSpec as P


NB = 128
CHAINS = 4
ADV = 4
PLANES = 8
QUADS = 4
COLS = 8
EACH = 32
WIDE = 256


def pieces_kernel(factors, out):
    for half in range(2):
        pieces = [factors[2 * half + a, c] for a in range(2) for c in range(CHAINS)]
        piece = jnp.concatenate(pieces, axis=1)
        for d in range(half, PLANES * QUADS, 2):
            out[d] = piece


def gather_kernel(place, b0, b1, b2, b3, out):
    for m, block in enumerate((b0, b1, b2, b3)):
        out[place[1] ^ m] = block[...]


def spread_kernel(pieces, out):
    turned = pieces[...].reshape(WIDE, WIDE).T
    for e in range(COLS):
        out[e] = turned


def split(x):
    high = x.astype(jnp.bfloat16)
    return high, (x - high.astype(jnp.float32)).astype(jnp.bfloat16)


def turned_factor(k, c, core, own, other):
    at = ((k % 2) * CHAINS + c) * 32
    picked = jnp.where(core == k // 2, own[:, at : at + 32, :], other[:, at : at + 32, :])
    return split(picked.reshape(WIDE, WIDE))


def dot(a, b, b_dim):
    return lax.dot_general(a, b, (((1,), (b_dim,)), ((), ())), preferred_element_type=jnp.float32)


def row_pass(panel, plane, first, last, starts, core, own, other):
    for k in range(ADV):
        for c in range(CHAINS):
            offset = lax.div(starts[k, c], NB) + 1 - QUADS * plane
            slot = (offset >= PLANES * QUADS).astype(jnp.int32)
            head = offset - PLANES * QUADS * slot

            @pl.when((head >= first) & (head <= last))
            def _():
                f_high, f_low = turned_factor(k, c, core, own, other)
                window = jnp.concatenate([panel[head, slot], panel[head + 1, slot]], axis=0)
                w_high, w_low = split(window)
                new = dot(f_high, w_high, 0) + (dot(f_low, w_high, 0) + dot(f_high, w_low, 0))
                panel[head, slot] = new[:NB]
                panel[head + 1, slot] = new[NB:]


def crossing(starts, first_block):
    found = jnp.int32(0)
    for k in range(ADV):
        for c in range(CHAINS):
            head = lax.div(starts[k, c], NB) + 1
            near = (head == first_block) | (head == first_block + PLANES * QUADS)
            found = found | near.astype(jnp.int32)
    return found == 1


def row_kernel(starts, place, lower, middle, upper, own, other, out, panel, side):
    core, plane = place[0], place[2]
    below = lax.rem(plane + PLANES - 1, PLANES)
    above = lax.rem(plane + 1, PLANES)
    into = crossing(starts, QUADS * plane)
    out_of = crossing(starts, QUADS * plane + QUADS)
    shift_low = (plane == 0).astype(jnp.int32)
    shift_high = (plane == PLANES - 1).astype(jnp.int32)

    @pl.when(into | (plane == 0))
    def _():
        side[1:5] = lower[...]
        row_pass(side, below, 1, 3, starts, core, own, other)
        panel[0, 0] = side[4, 0]
        panel[0, 1] = side[4, 1 - shift_low]

    @pl.when(out_of | (plane == PLANES - 1))
    def _():
        side[1:3] = upper[:2]

        @pl.when(lax.rem(above, PLANES // 2) == 0)
        def _():
            row_pass(side, above, 1, 1, starts, core, own, other)

        panel[5, 0] = side[1, shift_high]
        panel[5, 1] = side[1, 1]

    panel[1:5] = middle[...]
    row_pass(panel, plane, 0, 4, starts, core, own, other)
    out[...] = panel[1:5]


def col_kernel(starts, place, data, own, other, out):
    for q in range(QUADS):
        out[:, :, q * WIDE : (q + 1) * WIDE] = data[q]

    def spot(block):
        return lax.rem(block, COLS), pl.multiple_of(lax.div(block, COLS) * NB, NB)

    for k in range(ADV):
        results = []
        for c in range(CHAINS):
            head = lax.div(starts[k, c], NB)
            e0, o0 = spot(head)
            e1, o1 = spot(head + 1)
            window = jnp.concatenate([out[e0, :, pl.ds(o0, NB)], out[e1, :, pl.ds(o1, NB)]], axis=1)
            w_high, w_low = split(window)
            f_high, f_low = turned_factor(k, c, place[0], own, other)
            both = dot(jnp.concatenate([w_high, w_low], axis=0), f_high, 1)
            new = both[:EACH] + (both[EACH:] + dot(w_high, f_low, 1))
            results.append((e0, o0, e1, o1, new))
        for e0, o0, e1, o1, new in results:
            out[e0, :, pl.ds(o0, NB)] = new[:, :NB]
            out[e1, :, pl.ds(o1, NB)] = new[:, NB:]


SCALARS = pl.BlockSpec(memory_space=pltpu.SMEM)
VALUES = pl.BlockSpec(memory_space=pltpu.VMEM)


def kernel(body, scalars, inputs, out_shapes, scratch=()):
    outs = [jax.ShapeDtypeStruct(shape, jnp.float32) for shape in out_shapes]
    return pl.pallas_call(
        body,
        in_specs=[SCALARS] * scalars + [VALUES] * inputs,
        out_specs=[VALUES] * len(outs),
        out_shape=outs,
        scratch_shapes=[pltpu.VMEM(shape, jnp.float32) for shape in scratch],
    )


def local(matrix, starts, factors):
    z = lax.axis_index("planes")
    q = lax.axis_index("quads")
    place = jnp.stack([lax.rem(q, 2), q, z])
    tile = matrix.reshape(2, NB, QUADS * WIDE)
    quarters = [lax.dynamic_slice_in_dim(tile, (q ^ m) * WIDE, WIDE, 2) for m in range(QUADS)]
    blocks = [quarters[0]]
    for m in range(1, QUADS):
        blocks.append(lax.ppermute(quarters[m], "quads", [(i, i ^ m) for i in range(QUADS)]))
    (sent,) = kernel(pieces_kernel, 0, 1, [(PLANES * QUADS, 8, WIDE)])(factors)
    got = lax.all_to_all(sent, ("planes", "quads"), 0, 0, tiled=True)
    panel = (QUADS, 2, NB, WIDE)
    (middle,) = kernel(gather_kernel, 1, 4, [panel])(place, *blocks)
    lower = lax.ppermute(middle, "planes", [(i, (i + 1) % PLANES) for i in range(PLANES)])
    upper = lax.ppermute(middle, "planes", [(i, (i - 1) % PLANES) for i in range(PLANES)])
    (sent,) = kernel(spread_kernel, 0, 1, [(COLS, WIDE, WIDE)])(got)
    own = lax.all_to_all(sent, "cols", 0, 0, tiled=True)
    other = lax.ppermute(own, "quads", [(i, i ^ 1) for i in range(QUADS)])
    wide = [(QUADS + 2, 2, NB, WIDE), (QUADS + 1, 2, NB, WIDE)]
    (rows,) = kernel(row_kernel, 2, 5, [panel], wide)(
        starts, place, lower, middle, upper, own, other
    )
    rows = rows.reshape(QUADS * COLS, EACH, WIDE)
    came = lax.all_to_all(rows, ("quads", "cols"), 0, 0, tiled=True)
    came = came.reshape(QUADS, COLS, EACH, WIDE)
    (done,) = kernel(col_kernel, 2, 3, [(COLS, EACH, QUADS * WIDE)])(
        starts, place, came, own, other
    )
    home = lax.all_to_all(done, "cols", 0, 0, tiled=True)
    return home.reshape(2 * NB, QUADS * WIDE)


def solution(mesh):
    finer = Mesh(mesh.devices.reshape(PLANES, QUADS, COLS), ("planes", "quads", "cols"))
    rows = ("planes", "quads")
    in_specs = (P(rows, "cols"), P(), P(None, None, rows, "cols"))
    return jax.shard_map(
        local, mesh=finer, in_specs=in_specs, out_specs=P(rows, "cols"), check_vma=False
    )
```

```python
import jax
import jax.numpy as jnp
from jax import lax
from jax.experimental import pallas as pl
from jax.experimental.pallas import tpu as pltpu
from jax.sharding import Mesh
from jax.sharding import PartitionSpec as P


NB = 128
CHAINS = 4
ADV = 4
PLANES = 8
QUADS = 4
COLS = 8
EACH = 32
WIDE = 256


def pieces_kernel(factors, out):
    for half in range(2):
        pieces = [factors[2 * half + a, c] for a in range(2) for c in range(CHAINS)]
        piece = jnp.concatenate(pieces, axis=1)
        for d in range(half, PLANES * QUADS, 2):
            out[d] = piece


def gather_kernel(place, b0, b1, b2, b3, out, low):
    for m, block in enumerate((b0, b1, b2, b3)):
        out[place[1] ^ m] = block[...]
    low[...] = out[:2]


def spread_kernel(pieces, out):
    turned = pieces[...].reshape(WIDE, WIDE).T
    for e in range(COLS):
        out[e] = turned


def split(x):
    high = x.astype(jnp.bfloat16)
    return high, (x - high.astype(jnp.float32)).astype(jnp.bfloat16)


def turned_factor(k, c, core, own, other):
    at = ((k % 2) * CHAINS + c) * 32
    picked = jnp.where(core == k // 2, own[:, at : at + 32, :], other[:, at : at + 32, :])
    return split(picked.reshape(WIDE, WIDE))


def dot(a, b, b_dim):
    return lax.dot_general(a, b, (((1,), (b_dim,)), ((), ())), preferred_element_type=jnp.float32)


def row_pass(panel, plane, first, last, starts, core, own, other):
    for k in range(ADV):
        for c in range(CHAINS):
            offset = lax.div(starts[k, c], NB) + 1 - QUADS * plane
            slot = (offset >= PLANES * QUADS).astype(jnp.int32)
            head = offset - PLANES * QUADS * slot

            @pl.when((head >= first) & (head <= last))
            def _():
                f_high, f_low = turned_factor(k, c, core, own, other)
                window = jnp.concatenate([panel[head, slot], panel[head + 1, slot]], axis=0)
                w_high, w_low = split(window)
                new = dot(f_high, w_high, 0) + (dot(f_low, w_high, 0) + dot(f_high, w_low, 0))
                panel[head, slot] = new[:NB]
                panel[head + 1, slot] = new[NB:]


def crossing(starts, first_block):
    found = jnp.int32(0)
    for k in range(ADV):
        for c in range(CHAINS):
            head = lax.div(starts[k, c], NB) + 1
            near = (head == first_block) | (head == first_block + PLANES * QUADS)
            found = found | near.astype(jnp.int32)
    return found == 1


def row_kernel(starts, place, lower, middle, upper, own, other, out, panel, side):
    core, plane = place[0], place[2]
    below = lax.rem(plane + PLANES - 1, PLANES)
    above = lax.rem(plane + 1, PLANES)
    into = crossing(starts, QUADS * plane)
    out_of = crossing(starts, QUADS * plane + QUADS)
    shift_low = (plane == 0).astype(jnp.int32)
    shift_high = (plane == PLANES - 1).astype(jnp.int32)

    @pl.when(into | (plane == 0))
    def _():
        side[1:5] = lower[...]
        row_pass(side, below, 1, 3, starts, core, own, other)
        panel[0, 0] = side[4, 0]
        panel[0, 1] = side[4, 1 - shift_low]

    @pl.when(out_of | (plane == PLANES - 1))
    def _():
        side[1:3] = upper[...]

        @pl.when(lax.rem(above, PLANES // 2) == 0)
        def _():
            row_pass(side, above, 1, 1, starts, core, own, other)

        panel[5, 0] = side[1, shift_high]
        panel[5, 1] = side[1, 1]

    panel[1:5] = middle[...]
    row_pass(panel, plane, 0, 4, starts, core, own, other)
    out[...] = panel[1:5]


def col_kernel(starts, place, data, own, other, out):
    for q in range(QUADS):
        out[:, :, q * WIDE : (q + 1) * WIDE] = data[q]

    def spot(block):
        return lax.rem(block, COLS), pl.multiple_of(lax.div(block, COLS) * NB, NB)

    for k in range(ADV):
        results = []
        for c in range(CHAINS):
            head = lax.div(starts[k, c], NB)
            e0, o0 = spot(head)
            e1, o1 = spot(head + 1)
            window = jnp.concatenate([out[e0, :, pl.ds(o0, NB)], out[e1, :, pl.ds(o1, NB)]], axis=1)
            w_high, w_low = split(window)
            f_high, f_low = turned_factor(k, c, place[0], own, other)
            both = dot(jnp.concatenate([w_high, w_low], axis=0), f_high, 1)
            new = both[:EACH] + (both[EACH:] + dot(w_high, f_low, 1))
            results.append((e0, o0, e1, o1, new))
        for e0, o0, e1, o1, new in results:
            out[e0, :, pl.ds(o0, NB)] = new[:, :NB]
            out[e1, :, pl.ds(o1, NB)] = new[:, NB:]


SCALARS = pl.BlockSpec(memory_space=pltpu.SMEM)
VALUES = pl.BlockSpec(memory_space=pltpu.VMEM)


def kernel(body, scalars, inputs, out_shapes, scratch=()):
    outs = [jax.ShapeDtypeStruct(shape, jnp.float32) for shape in out_shapes]
    return pl.pallas_call(
        body,
        in_specs=[SCALARS] * scalars + [VALUES] * inputs,
        out_specs=[VALUES] * len(outs),
        out_shape=outs,
        scratch_shapes=[pltpu.VMEM(shape, jnp.float32) for shape in scratch],
        compiler_params=pltpu.CompilerParams(vmem_limit_bytes=24 << 20),
    )


def local(matrix, starts, factors):
    z = lax.axis_index("planes")
    q = lax.axis_index("quads")
    place = jnp.stack([lax.rem(q, 2), q, z])
    (sent,) = kernel(pieces_kernel, 0, 1, [(PLANES * QUADS, 8, WIDE)])(factors)
    got = lax.all_to_all(sent, ("planes", "quads"), 0, 0, tiled=True)
    tile = matrix.reshape(2, NB, QUADS * WIDE)
    quarters = [lax.dynamic_slice_in_dim(tile, (q ^ m) * WIDE, WIDE, 2) for m in range(QUADS)]
    blocks = [quarters[0]]
    for m in range(1, QUADS):
        blocks.append(lax.ppermute(quarters[m], "quads", [(i, i ^ m) for i in range(QUADS)]))
    (sent,) = kernel(spread_kernel, 0, 1, [(COLS, WIDE, WIDE)])(got)
    own = lax.all_to_all(sent, "cols", 0, 0, tiled=True)
    panel = (QUADS, 2, NB, WIDE)
    middle, low = kernel(gather_kernel, 1, 4, [panel, (2, 2, NB, WIDE)])(place, *blocks)
    lower = lax.ppermute(middle, "planes", [(i, (i + 1) % PLANES) for i in range(PLANES)])
    upper = lax.ppermute(low, "planes", [(i, (i - 1) % PLANES) for i in range(PLANES)])
    other = lax.ppermute(own, "quads", [(i, i ^ 1) for i in range(QUADS)])
    wide = [(QUADS + 2, 2, NB, WIDE), (QUADS + 1, 2, NB, WIDE)]
    (rows,) = kernel(row_kernel, 2, 5, [panel], wide)(
        starts, place, lower, middle, upper, own, other
    )
    rows = rows.reshape(QUADS * COLS, EACH, WIDE)
    came = lax.all_to_all(rows, ("quads", "cols"), 0, 0, tiled=True)
    came = came.reshape(QUADS, COLS, EACH, WIDE)
    (done,) = kernel(col_kernel, 2, 3, [(COLS, EACH, QUADS * WIDE)])(
        starts, place, came, own, other
    )
    home = lax.all_to_all(done, "cols", 0, 0, tiled=True)
    return home.reshape(2 * NB, QUADS * WIDE)


def solution(mesh):
    finer = Mesh(mesh.devices.reshape(PLANES, QUADS, COLS), ("planes", "quads", "cols"))
    rows = ("planes", "quads")
    in_specs = (P(rows, "cols"), P(), P(None, None, rows, "cols"))
    return jax.shard_map(
        local, mesh=finer, in_specs=in_specs, out_specs=P(rows, "cols"), check_vma=False
    )
```

```python
import jax
import jax.numpy as jnp
from jax import lax
from jax.experimental import pallas as pl
from jax.experimental.pallas import tpu as pltpu
from jax.sharding import Mesh
from jax.sharding import PartitionSpec as P


NB = 128
CHAINS = 4
ADV = 4
PLANES = 8
QUADS = 4
COLS = 8
EACH = 32
WIDE = 256


def pieces_kernel(factors, out):
    for half in range(2):
        pieces = [factors[2 * half + a, c] for a in range(2) for c in range(CHAINS)]
        piece = jnp.concatenate(pieces, axis=1)
        for d in range(half, PLANES * QUADS, 2):
            out[d] = piece


def gather_kernel(place, b0, b1, b2, b3, out, low):
    for m, block in enumerate((b0, b1, b2, b3)):
        out[place[1] ^ m] = block[...]
    low[...] = out[:2]


def spread_kernel(pieces, out):
    turned = pieces[...].reshape(WIDE, WIDE).T
    for e in range(COLS):
        out[e] = turned


def split(x):
    high = x.astype(jnp.bfloat16)
    return high, (x - high.astype(jnp.float32)).astype(jnp.bfloat16)


def turned_factor(k, c, core, own, other):
    at = ((k % 2) * CHAINS + c) * 32
    picked = jnp.where(core == k // 2, own[:, at : at + 32, :], other[:, at : at + 32, :])
    return split(picked.reshape(WIDE, WIDE))


def dot(a, b, b_dim):
    return lax.dot_general(a, b, (((1,), (b_dim,)), ((), ())), preferred_element_type=jnp.float32)


def row_pass(panel, plane, first, last, starts, core, own, other):
    for k in range(ADV):
        for c in range(CHAINS):
            offset = lax.div(starts[k, c], NB) + 1 - QUADS * plane
            slot = (offset >= PLANES * QUADS).astype(jnp.int32)
            head = offset - PLANES * QUADS * slot

            @pl.when((head >= first) & (head <= last))
            def _():
                f_high, f_low = turned_factor(k, c, core, own, other)
                window = jnp.concatenate([panel[head, slot], panel[head + 1, slot]], axis=0)
                w_high, w_low = split(window)
                new = dot(f_high, w_high, 0) + (dot(f_low, w_high, 0) + dot(f_high, w_low, 0))
                panel[head, slot] = new[:NB]
                panel[head + 1, slot] = new[NB:]


def crossing(starts, first_block):
    found = jnp.int32(0)
    for k in range(ADV):
        for c in range(CHAINS):
            head = lax.div(starts[k, c], NB) + 1
            near = (head == first_block) | (head == first_block + PLANES * QUADS)
            found = found | near.astype(jnp.int32)
    return found == 1


def row_kernel(starts, place, lower, middle, upper, own, other, out, panel, side):
    core, plane = place[0], place[2]
    below = lax.rem(plane + PLANES - 1, PLANES)
    above = lax.rem(plane + 1, PLANES)
    into = crossing(starts, QUADS * plane)
    out_of = crossing(starts, QUADS * plane + QUADS)
    shift_low = (plane == 0).astype(jnp.int32)
    shift_high = (plane == PLANES - 1).astype(jnp.int32)

    @pl.when(into | (plane == 0))
    def _():
        side[1:5] = lower[...]
        row_pass(side, below, 1, 3, starts, core, own, other)
        panel[0, 0] = side[4, 0]
        panel[0, 1] = side[4, 1 - shift_low]

    @pl.when(out_of | (plane == PLANES - 1))
    def _():
        side[1:3] = upper[...]

        @pl.when(lax.rem(above, PLANES // 2) == 0)
        def _():
            row_pass(side, above, 1, 1, starts, core, own, other)

        panel[5, 0] = side[1, shift_high]
        panel[5, 1] = side[1, 1]

    panel[1:5] = middle[...]
    row_pass(panel, plane, 0, 4, starts, core, own, other)
    for e in range(COLS):
        at = e % 4 * EACH
        out[e] = panel[1:5, e // 4, at : at + EACH, :]


def col_kernel(starts, place, data, own, other, out):
    for q in range(QUADS):
        out[:, :, q * WIDE : (q + 1) * WIDE] = data[:, q]

    def spot(block):
        return lax.rem(block, COLS), pl.multiple_of(lax.div(block, COLS) * NB, NB)

    for k in range(ADV):
        results = []
        for c in range(CHAINS):
            head = lax.div(starts[k, c], NB)
            e0, o0 = spot(head)
            e1, o1 = spot(head + 1)
            window = jnp.concatenate([out[e0, :, pl.ds(o0, NB)], out[e1, :, pl.ds(o1, NB)]], axis=1)
            w_high, w_low = split(window)
            f_high, f_low = turned_factor(k, c, place[0], own, other)
            both = dot(jnp.concatenate([w_high, w_low], axis=0), f_high, 1)
            new = both[:EACH] + (both[EACH:] + dot(w_high, f_low, 1))
            results.append((e0, o0, e1, o1, new))
        for e0, o0, e1, o1, new in results:
            out[e0, :, pl.ds(o0, NB)] = new[:, :NB]
            out[e1, :, pl.ds(o1, NB)] = new[:, NB:]


SCALARS = pl.BlockSpec(memory_space=pltpu.SMEM)
VALUES = pl.BlockSpec(memory_space=pltpu.VMEM)


def kernel(body, scalars, inputs, out_shapes, scratch=()):
    outs = [jax.ShapeDtypeStruct(shape, jnp.float32) for shape in out_shapes]
    return pl.pallas_call(
        body,
        in_specs=[SCALARS] * scalars + [VALUES] * inputs,
        out_specs=[VALUES] * len(outs),
        out_shape=outs,
        scratch_shapes=[pltpu.VMEM(shape, jnp.float32) for shape in scratch],
        compiler_params=pltpu.CompilerParams(vmem_limit_bytes=24 << 20),
    )


def local(matrix, starts, factors):
    z = lax.axis_index("planes")
    q = lax.axis_index("quads")
    place = jnp.stack([lax.rem(q, 2), q, z])
    (sent,) = kernel(pieces_kernel, 0, 1, [(PLANES * QUADS, 8, WIDE)])(factors)
    got = lax.all_to_all(sent, ("planes", "quads"), 0, 0, tiled=True)
    tile = matrix.reshape(2, NB, QUADS * WIDE)
    quarters = [lax.dynamic_slice_in_dim(tile, (q ^ m) * WIDE, WIDE, 2) for m in range(QUADS)]
    blocks = [quarters[0]]
    for m in range(1, QUADS):
        blocks.append(lax.ppermute(quarters[m], "quads", [(i, i ^ m) for i in range(QUADS)]))
    (sent,) = kernel(spread_kernel, 0, 1, [(COLS, WIDE, WIDE)])(got)
    own = lax.all_to_all(sent, "cols", 0, 0, tiled=True)
    panel = (QUADS, 2, NB, WIDE)
    middle, low = kernel(gather_kernel, 1, 4, [panel, (2, 2, NB, WIDE)])(place, *blocks)
    lower = lax.ppermute(middle, "planes", [(i, (i + 1) % PLANES) for i in range(PLANES)])
    upper = lax.ppermute(low, "planes", [(i, (i - 1) % PLANES) for i in range(PLANES)])
    other = lax.ppermute(own, "quads", [(i, i ^ 1) for i in range(QUADS)])
    wide = [(QUADS + 2, 2, NB, WIDE), (QUADS + 1, 2, NB, WIDE)]
    (rows,) = kernel(row_kernel, 2, 5, [(COLS, QUADS, EACH, WIDE)], wide)(
        starts, place, lower, middle, upper, own, other
    )
    rows = rows.reshape(QUADS * COLS, EACH, WIDE)
    came = lax.all_to_all(rows, ("cols", "quads"), 0, 0, tiled=True)
    came = came.reshape(COLS, QUADS, EACH, WIDE)
    (done,) = kernel(col_kernel, 2, 3, [(COLS, EACH, QUADS * WIDE)])(
        starts, place, came, own, other
    )
    home = lax.all_to_all(done, "cols", 0, 0, tiled=True)
    return home.reshape(2 * NB, QUADS * WIDE)


def solution(mesh):
    finer = Mesh(mesh.devices.reshape(PLANES, QUADS, COLS), ("planes", "quads", "cols"))
    rows = ("planes", "quads")
    in_specs = (P(rows, "cols"), P(), P(None, None, rows, "cols"))
    return jax.shard_map(
        local, mesh=finer, in_specs=in_specs, out_specs=P(rows, "cols"), check_vma=False
    )
```
